32 devices in a mesh: seq: 16 (over z, y, x), head: 2 (over core).
Axes of the slice: x: 2, y: 2, z: 4, core: 2. Of those that a mesh axis runs over, the one named last changes fastest.
Arguments:
- queries: bfloat16 [2048, 64, 512], P('seq', 'head'), may hold values from -1000 to 1000
- cotangent: bfloat16 [2048, 64, 512], P('seq', 'head'), may hold values from -6 to 6
- window_kv: bfloat16 [2048, 512], P('seq'), may hold values from -6 to 6
- context: bfloat16 [4096, 512], P(('seq', 'head')), may hold values from -6 to 6
- pool_weight: float32 [128, 512], replicated, may hold values from -0.5 to 0.5
Outputs:
- attn_out: bfloat16 [2048, 64, 512], P('seq', 'head')
- grad_queries: bfloat16 [2048, 64, 512], P('seq', 'head')
- grad_context: float32 [4096, 512], P(('seq', 'head'))
The draws below stay inside these ranges and needn't reach their ends.
All inputs are finite; a program needn't handle non-finite values.
Results may differ from the reference program's by a relative error of at most 0.0074.
Values may be sent and summed in bfloat16 or wider, within the bound.
No kernel may reach another device: no remote copies, remote signals or barrier semaphores. Data moves between devices by JAX's collectives and lax.ppermute only.
A program may use at most 64 MiB of HBM per device.

```python
import jax
import jax.numpy as jnp
from jax import lax

HEADS = 64
DH = 512
POOL = 128
WINDOW = 128
Q_DEV = 128
QUERIES = 2048
COMPRESSED = 32
CONTEXT = 4096
N_SEQ = 16


def window_rows(key):
    return jnp.clip(jax.random.normal(jax.random.fold_in(key, 101), (QUERIES, DH), jnp.float32), -6.0, 6.0)


def draw_window_kv(key, part):
    return window_rows(key).astype(jnp.bfloat16)


def draw_queries(key, part):
    draw_key = jax.random.fold_in(key, 202)
    drawn = 2.0 * jnp.clip(jax.random.normal(draw_key, (QUERIES, HEADS, DH), jnp.float32), -4.0, 4.0)
    return drawn.astype(jnp.bfloat16)


def steps_of(own_key, extent, shards, least, largest):
    level, own = 1.0, jax.random.fold_in(own_key, 6)
    for dim, parts in shards:
        heights = jnp.exp(jax.random.uniform(jax.random.fold_in(own, dim), (parts,), jnp.float32, least / len(shards), largest / len(shards)))
        level = level * jnp.repeat(heights, extent[dim] // parts).reshape([-1 if axis == dim else 1 for axis in range(len(extent))])
    return level


def scatter_about(own_key, dims, scale, bound, pieces=(), held_as=jnp.bfloat16):
    array = scale * jax.random.normal(own_key, dims, jnp.float32)
    if pieces:
        array = array * steps_of(own_key, dims, pieces, -0.22, 0.18)
    return jnp.clip(array, -bound, bound).astype(held_as)


def setup_inputs(seed: int = 0) -> dict:
    streams_of = jax.random.split(jax.random.key(seed), 6)
    return {
        "queries": draw_queries(jax.random.fold_in(streams_of[5], 71), 0),
        "cotangent": scatter_about(streams_of[1], (QUERIES, HEADS, DH), 1.0, 6.0, ((0, 16), (1, 2))),
        "window_kv": draw_window_kv(jax.random.fold_in(streams_of[5], 71), 0),
        "context": scatter_about(streams_of[3], (CONTEXT, DH), 1.0, 6.0, ((0, 32),)),
        "pool_weight": scatter_about(streams_of[4], (POOL, DH), POOL ** -0.5, 0.5, (), jnp.float32),
    }


def attend(queries, cotangent, comp_keys, window_keys, query_pos, key_pos):
    factor = DH ** (-0.5)
    valid = (key_pos[None, :] <= query_pos[:, None]) & (key_pos[None, :] > query_pos[:, None] - WINDOW) & (key_pos[None, :] >= 0)
    scores_comp = factor * jnp.einsum('qhd,kd->qhk', queries, comp_keys)
    scores_win = factor * jnp.einsum('qhd,kd->qhk', queries, window_keys)
    scores_win = jnp.where(valid[:, None, :], scores_win, -1e+30)
    peak = jnp.maximum(lax.optimization_barrier(jnp.max(scores_comp, -1, keepdims=True)), lax.optimization_barrier(jnp.max(scores_win, -1, keepdims=True)))
    exp_comp = jnp.exp(scores_comp - peak)
    exp_win = jnp.exp(scores_win - peak)
    total = lax.optimization_barrier(jnp.sum(exp_comp, -1, keepdims=True)) + lax.optimization_barrier(jnp.sum(exp_win, -1, keepdims=True))
    prob_comp = exp_comp / total
    prob_win = exp_win / total
    half_comp = lax.optimization_barrier(prob_comp.astype(jnp.bfloat16)).astype(jnp.float32)
    half_win = lax.optimization_barrier(prob_win.astype(jnp.bfloat16)).astype(jnp.float32)
    out_full = jnp.einsum('qhk,kd->qhd', half_comp, comp_keys) + jnp.einsum('qhk,kd->qhd', half_win, window_keys)
    grad_prob_comp = jnp.einsum('qhd,kd->qhk', cotangent, comp_keys)
    grad_prob_win = jnp.einsum('qhd,kd->qhk', cotangent, window_keys)
    row_delta = lax.optimization_barrier(jnp.sum(cotangent * out_full, -1, keepdims=True))
    score_comp = lax.optimization_barrier((prob_comp * (grad_prob_comp - row_delta)).astype(jnp.bfloat16)).astype(jnp.float32)
    score_win = lax.optimization_barrier((prob_win * (grad_prob_win - row_delta)).astype(jnp.bfloat16)).astype(jnp.float32)
    grad_queries = factor * (jnp.einsum('qhk,kd->qhd', score_comp, comp_keys) + jnp.einsum('qhk,kd->qhd', score_win, window_keys))
    grad_comp = jnp.einsum('qhk,qhd->kd', half_comp, cotangent) + factor * jnp.einsum('qhk,qhd->kd', score_comp, queries)
    return (out_full, grad_queries, grad_comp)

def reference(queries, cotangent, window_kv, context, pool_weight):
    blocks = context.astype(jnp.float32).reshape(COMPRESSED, POOL, DH)
    pooled = lax.optimization_barrier(jnp.sum(blocks * pool_weight[None], axis=1))
    inverse = lax.rsqrt(lax.optimization_barrier(jnp.mean(pooled * pooled, -1, keepdims=True)) + 1e-06)
    normed = pooled * inverse
    comp_keys = lax.optimization_barrier(normed.astype(jnp.bfloat16)).astype(jnp.float32)
    padded = jnp.concatenate([jnp.zeros((WINDOW, DH), jnp.bfloat16), window_kv], 0).astype(jnp.float32)

    def step(grad_total, block_index):
        offset = block_index * Q_DEV
        query_block = lax.dynamic_slice_in_dim(queries, offset, Q_DEV, 0).astype(jnp.float32)
        grad_block = lax.dynamic_slice_in_dim(cotangent, offset, Q_DEV, 0).astype(jnp.float32)
        window_keys = lax.dynamic_slice_in_dim(padded, offset, Q_DEV + WINDOW, 0)
        query_pos = offset + jnp.arange(Q_DEV, dtype=jnp.int32)
        key_pos = offset - WINDOW + jnp.arange(Q_DEV + WINDOW, dtype=jnp.int32)
        out_full, grad_rows, grad_comp = attend(query_block, grad_block, comp_keys, window_keys, query_pos, key_pos)
        return (grad_total + grad_comp, (out_full.astype(jnp.bfloat16), grad_rows.astype(jnp.bfloat16)))
    grad_total, (outputs, grad_rows) = lax.scan(step, jnp.zeros((COMPRESSED, DH), jnp.float32), jnp.arange(N_SEQ, dtype=jnp.int32))
    attn_out = outputs.reshape(QUERIES, HEADS, DH)
    grad_queries = grad_rows.reshape(QUERIES, HEADS, DH)
    grad_pooled = inverse * (grad_total - normed * lax.optimization_barrier(jnp.mean(grad_total * normed, -1, keepdims=True)))
    grad_context = (pool_weight[None] * grad_pooled[:, None, :]).reshape(CONTEXT, DH)
    return (attn_out, grad_queries, grad_context)
```

```python
import functools

import jax
import jax.numpy as jnp
from jax import lax
from jax.experimental import pallas as pl
from jax.experimental.pallas import tpu as pltpu
from jax.sharding import PartitionSpec as P

POOL = 128
WINDOW = 128
TILE = 16
AXES = ("seq", "head")
LOG2E = 1.4426950408889634
NT = (((1,), (1,)), ((), ()))
TN = (((0,), (0,)), ((), ()))


def whole(shape):
    return pl.BlockSpec(shape, lambda *_: (0,) * len(shape))


def pool_kernel(context_ref, weight_ref, pooled_ref, send_ref):
    rows = pooled_ref.shape[0]
    copies = send_ref.shape[0] // rows
    parts = []
    for block in range(rows):
        entries = context_ref[pl.ds(block * POOL, POOL), :].astype(jnp.float32)
        parts.append(jnp.sum(entries * weight_ref[...], axis=0, keepdims=True))
    pooled = parts[0] if rows == 1 else jnp.concatenate(parts, 0)
    pooled_ref[...] = pooled
    inverse = lax.rsqrt(jnp.mean(pooled * pooled, -1, keepdims=True) + 1e-06)
    normed = pooled * inverse
    if rows == 1:
        spread = jnp.broadcast_to(normed, send_ref.shape)
    else:
        spread = jnp.concatenate([normed] * copies, 0)
    send_ref[...] = spread.astype(jnp.bfloat16)


def finish_kernel(parts_ref, pooled_ref, weight_ref, out_ref):
    rows, width = pooled_ref.shape
    copies = parts_ref.shape[0] // rows
    parts = parts_ref[...]
    if rows == 1:
        total = jnp.sum(parts, axis=0, keepdims=True)
    else:
        total = jnp.sum(parts.reshape(copies, rows, width), axis=0)
    pooled = pooled_ref[...]
    inverse = lax.rsqrt(jnp.mean(pooled * pooled, -1, keepdims=True) + 1e-06)
    normed = pooled * inverse
    grad = inverse * (total - normed * jnp.mean(total * normed, -1, keepdims=True))
    for block in range(rows):
        out_ref[pl.ds(block * POOL, POOL), :] = weight_ref[...] * grad[block : block + 1, :]


def fill_keys(step, comp_ref, prev_ref, cur_ref, window_ref, keys_ref):
    count = comp_ref.shape[0]

    @pl.when(step == 0)
    def _():
        window_ref[pl.ds(0, WINDOW), :] = prev_ref[...]
        window_ref[pl.ds(WINDOW, cur_ref.shape[0]), :] = cur_ref[...]
        keys_ref[pl.ds(0, count), :] = comp_ref[...]

    start = pl.multiple_of(step * TILE, TILE)
    keys_ref[pl.ds(count, TILE + WINDOW), :] = window_ref[pl.ds(start, TILE + WINDOW), :]


def score_kernel(heads, first_ref, q_ref, c_ref, comp_ref, prev_ref, cur_ref, p_ref, g_ref, sum_ref, window_ref, keys_ref):
    step = pl.program_id(0)
    count = comp_ref.shape[0]
    rows, width = q_ref.shape
    factor = width ** (-0.5)
    fill_keys(step, comp_ref, prev_ref, cur_ref, window_ref, keys_ref)
    keys = keys_ref[...]
    chunk = min(256, rows)
    slab = TILE + WINDOW
    low = jnp.where(first_ref[0] > 0, WINDOW - step * TILE, 0)
    total = jnp.zeros(sum_ref.shape, jnp.float32)
    for at in range(0, rows, chunk):
        q = q_ref[pl.ds(at, chunk), :]
        c = c_ref[pl.ds(at, chunk), :]
        scores = lax.dot_general(keys, q, NT, preferred_element_type=jnp.float32)
        grads = lax.dot_general(keys, c, NT, preferred_element_type=jnp.float32)
        key = lax.broadcasted_iota(jnp.int32, (slab, chunk), 0)
        token = (lax.broadcasted_iota(jnp.int32, (slab, chunk), 1) + at) // heads
        valid = (key > token) & (key <= token + WINDOW) & (key >= low)
        scores = jnp.concatenate([scores[:count], jnp.where(valid, scores[count:], -1e30)], 0)
        peak = jnp.max(scores, 0, keepdims=True)
        weights = jnp.exp2((scores - peak) * (factor * LOG2E))
        probs = weights * (1.0 / jnp.sum(weights, 0, keepdims=True))
        half = probs.astype(jnp.bfloat16)
        delta = jnp.sum(half.astype(jnp.float32) * grads, 0, keepdims=True)
        slope = (probs * (grads - delta)).astype(jnp.bfloat16)
        p_ref[0, :, pl.ds(at, chunk)] = half
        g_ref[0, :, pl.ds(at, chunk)] = slope
        total += jnp.dot(half[:count], c, preferred_element_type=jnp.float32)
        total += factor * jnp.dot(slope[:count], q, preferred_element_type=jnp.float32)

    @pl.when(step == 0)
    def _():
        sum_ref[...] = total

    @pl.when(step > 0)
    def _():
        sum_ref[...] += total


def output_kernel(p_ref, g_ref, comp_ref, prev_ref, cur_ref, out_ref, grad_ref, window_ref, keys_ref):
    step = pl.program_id(0)
    fill_keys(step, comp_ref, prev_ref, cur_ref, window_ref, keys_ref)
    rows, width = out_ref.shape
    factor = width ** (-0.5)
    keys = keys_ref[...]
    chunk = min(256, rows)
    for at in range(0, rows, chunk):
        half = p_ref[0, :, pl.ds(at, chunk)]
        slope = g_ref[0, :, pl.ds(at, chunk)]
        out = lax.dot_general(half, keys, TN, preferred_element_type=jnp.float32)
        out_ref[pl.ds(at, chunk), :] = out.astype(jnp.bfloat16)
        grad = lax.dot_general(slope, keys, TN, preferred_element_type=jnp.float32)
        grad_ref[pl.ds(at, chunk), :] = (grad * factor).astype(jnp.bfloat16)


def local(queries, cotangent, window_kv, context, pool_weight):
    tokens, heads, width = queries.shape
    pool_rows = context.shape[0] // POOL
    devices = lax.axis_size("seq") * lax.axis_size("head")
    count = devices * pool_rows
    rows = tokens * heads
    steps = tokens // TILE
    block = TILE * heads
    slab = count + TILE + WINDOW

    pooled, send = pl.pallas_call(
        pool_kernel,
        out_shape=(
            jax.ShapeDtypeStruct((pool_rows, width), jnp.float32),
            jax.ShapeDtypeStruct((count, width), jnp.bfloat16),
        ),
        name="pool",
    )(context, pool_weight)
    comp = lax.all_to_all(send, AXES, 0, 0, tiled=True)
    size = lax.axis_size("seq")
    prev = lax.ppermute(window_kv[-WINDOW:], "seq", [(i, i + 1) for i in range(size - 1)])
    first = (lax.axis_index("seq") == 0).astype(jnp.int32).reshape(1)

    q = queries.reshape(rows, width)
    c = cotangent.reshape(rows, width)
    tile = pl.BlockSpec((block, width), lambda i: (i, 0))
    probs = pl.BlockSpec((1, slab, block), lambda i: (i, 0, 0))
    keys = [whole((count, width)), whole((WINDOW, width)), whole((tokens, width))]
    scratch = [
        pltpu.VMEM((WINDOW + tokens, width), jnp.bfloat16),
        pltpu.VMEM((slab, width), jnp.bfloat16),
    ]
    kept = jax.ShapeDtypeStruct((steps, slab, block), jnp.bfloat16)
    half, slope, grad_comp = pl.pallas_call(
        functools.partial(score_kernel, heads),
        grid=(steps,),
        in_specs=[pl.BlockSpec(memory_space=pltpu.SMEM), tile, tile, *keys],
        out_specs=(probs, probs, whole((count, width))),
        out_shape=(kept, kept, jax.ShapeDtypeStruct((count, width), jnp.float32)),
        scratch_shapes=scratch,
        cost_estimate=pl.CostEstimate(
            flops=4 * rows * slab * width + 4 * rows * count * width,
            bytes_accessed=4 * rows * (width + slab),
            transcendentals=rows * slab,
        ),
        name="score",
    )(first, q, c, comp, prev, window_kv)
    parts = lax.all_to_all(grad_comp, AXES, 0, 0, tiled=True)
    out, grad = pl.pallas_call(
        output_kernel,
        grid=(steps,),
        in_specs=[probs, probs, *keys],
        out_specs=(tile, tile),
        out_shape=(jax.ShapeDtypeStruct((rows, width), jnp.bfloat16),) * 2,
        scratch_shapes=scratch,
        cost_estimate=pl.CostEstimate(
            flops=4 * rows * slab * width,
            bytes_accessed=4 * rows * (width + slab),
            transcendentals=0,
        ),
        name="outputs",
    )(half, slope, comp, prev, window_kv)
    grad_context = pl.pallas_call(
        finish_kernel,
        out_shape=jax.ShapeDtypeStruct(context.shape, jnp.float32),
        name="finish",
    )(parts, pooled, pool_weight)
    return out.reshape(queries.shape), grad.reshape(queries.shape), grad_context


def solution(mesh):
    in_specs = (
        P("seq", "head", None),
        P("seq", "head", None),
        P("seq", None),
        P(("seq", "head"), None),
        P(),
    )
    out_specs = (P("seq", "head", None), P("seq", "head", None), P(("seq", "head"), None))
    return jax.shard_map(local, mesh=mesh, in_specs=in_specs, out_specs=out_specs, check_vma=False)
```

```python
import functools

import jax
import jax.numpy as jnp
from jax import lax
from jax.experimental import pallas as pl
from jax.experimental.pallas import tpu as pltpu
from jax.sharding import PartitionSpec as P


POOL = 128
WINDOW = 128
LANES = 128
GROUP = 2
TILE = 16
AXES = ("seq", "head")
LOG2E = 1.4426950408889634
MIB = 1 << 20
NT = (((1,), (1,)), ((), ()))
TN = (((0,), (0,)), ((), ()))
HBM = pl.BlockSpec(memory_space=pltpu.HBM)
VMEM = pl.BlockSpec(memory_space=pltpu.VMEM)
SMEM = pl.BlockSpec(memory_space=pltpu.SMEM)


def hbm(value):
    return pltpu.with_memory_space_constraint(value, pltpu.HBM)


def vmem(value):
    return pltpu.with_memory_space_constraint(value, pltpu.VMEM)


def pool_kernel(context_hbm, weight_hbm, pooled_ref, send_ref, context_ref, weight_ref, sem):
    blocks, width = pooled_ref.shape
    copies = (
        pltpu.make_async_copy(context_hbm, context_ref, sem.at[0]),
        pltpu.make_async_copy(weight_hbm, weight_ref, sem.at[1]),
    )
    for copy in copies:
        copy.start()
    for copy in copies:
        copy.wait()
    for block in range(blocks):
        entries = context_ref[pl.ds(block * POOL, POOL), :].astype(jnp.float32)
        pooled = jnp.sum(entries * weight_ref[...], axis=0, keepdims=True)
        pooled_ref[pl.ds(block, 1), :] = pooled
        normed = pooled * lax.rsqrt(jnp.mean(pooled * pooled, -1, keepdims=True) + 1e-06)
        lines = jnp.concatenate([normed[:, at : at + LANES] for at in range(0, width, LANES)], 0)
        if blocks == 1:
            send_ref[...] = jnp.broadcast_to(lines[None], send_ref.shape)
        else:
            for peer in range(send_ref.shape[0] // blocks):
                send_ref[peer * blocks + block] = lines


def finish_kernel(parts_ref, pooled_ref, weight_ref, out_ref):
    blocks, _ = pooled_ref.shape
    count, lines, lanes = parts_ref.shape
    total = jnp.sum(parts_ref[...].reshape(count // blocks, blocks, lines, lanes), 0)
    for block in range(blocks):
        grad = jnp.concatenate([total[block, j : j + 1] for j in range(lines)], 1)
        pooled = pooled_ref[pl.ds(block, 1), :]
        inverse = lax.rsqrt(jnp.mean(pooled * pooled, -1, keepdims=True) + 1e-06)
        normed = pooled * inverse
        grad = inverse * (grad - normed * jnp.mean(grad * normed, -1, keepdims=True))
        out_ref[pl.ds(block * POOL, POOL), :] = weight_ref[...] * grad


def fill_keys(comp_ref, prev_ref, window_ref, *keys_refs):
    count, lines, lanes = comp_ref.shape
    window_ref[pl.ds(0, WINDOW), :] = prev_ref[...]
    for line in range(lines):
        piece = comp_ref[:, line, :].astype(jnp.bfloat16)
        for keys_ref in keys_refs:
            keys_ref[pl.ds(0, count), pl.ds(line * lanes, lanes)] = piece


def score_kernel(
    heads, first_ref, q_hbm, c_hbm, comp_ref, prev_ref, cur_hbm, p_ref, g_ref, sum_ref,
    q_ref, c_ref, window_ref, keys_ref, total_ref, sem, cur_sem,
):
    count, lines, lanes = comp_ref.shape
    rows, width = q_ref.shape
    part = TILE * heads
    group = min(GROUP, p_ref.shape[0])
    block = part * group
    steps = rows // block
    slab = TILE * group + WINDOW
    factor = width ** (-0.5)

    def fetch(step):
        span = pl.ds(pl.multiple_of(step * block, block), block)
        return (
            pltpu.make_async_copy(q_hbm.at[span], q_ref.at[span], sem.at[0, step]),
            pltpu.make_async_copy(c_hbm.at[span], c_ref.at[span], sem.at[1, step]),
        )

    copy_cur = pltpu.make_async_copy(cur_hbm, window_ref.at[pl.ds(WINDOW, cur_hbm.shape[0])], cur_sem)
    copy_cur.start()
    for step in range(steps):
        for copy in fetch(step):
            copy.start()
    fill_keys(comp_ref, prev_ref, window_ref, keys_ref)
    total_ref[...] = jnp.zeros_like(total_ref)
    copy_cur.wait()

    @pl.loop(0, steps)
    def _(step):
        start = pl.multiple_of(step * (TILE * group), TILE * group)
        keys_ref[pl.ds(count, slab), :] = window_ref[pl.ds(start, slab), :]
        for copy in fetch(step):
            copy.wait()
        keys = keys_ref[...]
        span = pl.ds(pl.multiple_of(step * block, block), block)
        q = q_ref[span, :]
        c = c_ref[span, :]
        scores = lax.dot_general(keys, q, NT, preferred_element_type=jnp.float32)
        grads = lax.dot_general(keys, c, NT, preferred_element_type=jnp.float32)
        key = lax.broadcasted_iota(jnp.int32, (slab, block), 0)
        token = lax.broadcasted_iota(jnp.int32, (slab, block), 1) // heads
        low = jnp.where(first_ref[0] > 0, WINDOW - start, 0)
        valid = (key > token) & (key <= token + WINDOW) & (key >= low)
        scores = jnp.concatenate([scores[:count], jnp.where(valid, scores[count:], -1e30)], 0)
        peak = jnp.max(scores, 0, keepdims=True)
        weights = jnp.exp2((scores - peak) * (factor * LOG2E))
        probs = weights * (1.0 / jnp.sum(weights, 0, keepdims=True))
        half = probs.astype(jnp.bfloat16)
        delta = jnp.sum(half.astype(jnp.float32) * grads, 0, keepdims=True)
        slope = (probs * (grads - delta)).astype(jnp.bfloat16)
        for ref, value in ((p_ref, half), (g_ref, slope)):
            for index in range(group):
                columns = slice(index * part, (index + 1) * part)
                first = count + index * TILE
                ref[step * group + index, pl.ds(0, count), :] = value[:count, columns]
                window = value[first : first + TILE + WINDOW, columns]
                ref[step * group + index, pl.ds(count, TILE + WINDOW), :] = window
        total = jnp.dot(half[:count], c, preferred_element_type=jnp.float32)
        total += factor * jnp.dot(slope[:count], q, preferred_element_type=jnp.float32)
        total_ref[...] += total

    for line in range(lines):
        sum_ref[:, line, :] = total_ref[:, pl.ds(line * lanes, lanes)]


def output_kernel(
    p_ref, g_ref, comp_ref, prev_ref, cur_hbm, out_hbm, grad_hbm,
    out_ref, grad_ref, window_ref, keys_refs, sem, cur_sem,
):
    steps, _, block = p_ref.shape
    count = comp_ref.shape[0]
    factor = out_ref.shape[1] ** (-0.5)
    unroll = 2 if steps % 2 == 0 else 1

    def flush(step):
        rows = pl.ds(pl.multiple_of(step * block, block), block)
        return (
            pltpu.make_async_copy(out_ref.at[rows], out_hbm.at[rows], sem.at[0, step]),
            pltpu.make_async_copy(grad_ref.at[rows], grad_hbm.at[rows], sem.at[1, step]),
        )

    copy_cur = pltpu.make_async_copy(cur_hbm, window_ref.at[pl.ds(WINDOW, cur_hbm.shape[0])], cur_sem)
    copy_cur.start()
    fill_keys(comp_ref, prev_ref, window_ref, keys_refs.at[0], keys_refs.at[1])
    copy_cur.wait()

    @pl.loop(0, steps // unroll)
    def _(turn):
        for slot in range(unroll):
            step = turn * unroll + slot
            start = pl.multiple_of(step * TILE, TILE)
            keys_refs[slot, pl.ds(count, TILE + WINDOW), :] = window_ref[pl.ds(start, TILE + WINDOW), :]
            keys = keys_refs[slot]
            rows = pl.ds(pl.multiple_of(step * block, block), block)
            out = lax.dot_general(p_ref[step], keys, TN, preferred_element_type=jnp.float32)
            out_ref[rows, :] = out.astype(jnp.bfloat16)
            grad = lax.dot_general(g_ref[step], keys, TN, preferred_element_type=jnp.float32)
            grad_ref[rows, :] = (grad * factor).astype(jnp.bfloat16)
        for slot in range(unroll):
            for copy in flush(turn * unroll + slot):
                copy.start()

    for step in range(steps):
        for copy in flush(step):
            copy.wait()


def local(queries, cotangent, window_kv, context, pool_weight):
    tokens, heads, width = queries.shape
    blocks = context.shape[0] // POOL
    size = lax.axis_size("seq")
    count = size * lax.axis_size("head") * blocks
    rows = tokens * heads
    steps = tokens // TILE
    block = TILE * heads
    slab = count + TILE + WINDOW
    lines = width // LANES

    packed = jax.ShapeDtypeStruct((count, lines, LANES), jnp.float32)
    pooled, send = pl.pallas_call(
        pool_kernel,
        in_specs=[HBM, HBM],
        out_specs=(VMEM, VMEM),
        out_shape=(jax.ShapeDtypeStruct((blocks, width), jnp.float32), packed),
        scratch_shapes=[
            pltpu.VMEM(context.shape, context.dtype),
            pltpu.VMEM(pool_weight.shape, pool_weight.dtype),
            pltpu.SemaphoreType.DMA((2,)),
        ],
        name="pool",
        compiler_params=pltpu.CompilerParams(vmem_limit_bytes=8 * MIB),
    )(hbm(context), hbm(pool_weight))
    comp = lax.all_to_all(send, AXES, 0, 0, tiled=True)
    prev = lax.ppermute(window_kv[-WINDOW:], "seq", [(i, i + 1) for i in range(size - 1)])
    first = (lax.axis_index("seq") == 0).astype(jnp.int32).reshape(1)

    q = hbm(queries.reshape(rows, width))
    c = hbm(cotangent.reshape(rows, width))
    cur = hbm(window_kv)
    full = pltpu.VMEM((rows, width), jnp.bfloat16)
    kept = pltpu.VMEM((steps, slab, block), jnp.bfloat16)
    group = min(GROUP, steps)
    window = pltpu.VMEM((WINDOW + tokens, width), jnp.bfloat16)
    wide = pltpu.VMEM((count + TILE * group + WINDOW, width), jnp.bfloat16)
    total = pltpu.VMEM((count, width), jnp.float32)
    params = pltpu.CompilerParams(vmem_limit_bytes=32 * MIB)
    half, slope, grad_comp = pl.pallas_call(
        functools.partial(score_kernel, heads),
        in_specs=[SMEM, HBM, HBM, VMEM, VMEM, HBM],
        out_specs=(VMEM, VMEM, VMEM),
        out_shape=(kept, kept, packed),
        scratch_shapes=[full, full, window, wide, total, pltpu.SemaphoreType.DMA((2, steps // group)), pltpu.SemaphoreType.DMA],
        cost_estimate=pl.CostEstimate(
            flops=4 * rows * slab * width + 4 * rows * count * width,
            bytes_accessed=4 * rows * (width + slab),
            transcendentals=rows * slab,
        ),
        compiler_params=params,
        name="score",
    )(first, q, c, comp, prev, cur)
    parts = lax.all_to_all(grad_comp, AXES, 0, 0, tiled=True)
    out, grad = pl.pallas_call(
        output_kernel,
        in_specs=[VMEM, VMEM, VMEM, VMEM, HBM],
        out_specs=(HBM, HBM),
        out_shape=(jax.ShapeDtypeStruct((rows, width), jnp.bfloat16),) * 2,
        scratch_shapes=[full, full, window, pltpu.VMEM((2, slab, width), jnp.bfloat16), pltpu.SemaphoreType.DMA((2, steps)), pltpu.SemaphoreType.DMA],
        cost_estimate=pl.CostEstimate(
            flops=4 * rows * slab * width,
            bytes_accessed=4 * rows * (width + slab),
            transcendentals=0,
        ),
        compiler_params=params,
        name="outputs",
    )(vmem(half), vmem(slope), comp, prev, cur)
    grad_context = pl.pallas_call(
        finish_kernel,
        out_shape=jax.ShapeDtypeStruct(context.shape, jnp.float32),
        name="finish",
        compiler_params=pltpu.CompilerParams(vmem_limit_bytes=8 * MIB),
    )(parts, pooled, pool_weight)
    return out.reshape(queries.shape), grad.reshape(queries.shape), grad_context


def solution(mesh):
    in_specs = (
        P("seq", "head", None),
        P("seq", "head", None),
        P("seq", None),
        P(("seq", "head"), None),
        P(),
    )
    out_specs = (P("seq", "head", None), P("seq", "head", None), P(("seq", "head"), None))

    return jax.shard_map(local, mesh=mesh, in_specs=in_specs, out_specs=out_specs, check_vma=False)
```

```python
import functools

import jax
import jax.numpy as jnp
from jax import lax
from jax.experimental import pallas as pl
from jax.experimental.pallas import tpu as pltpu
from jax.sharding import PartitionSpec as P


POOL = 128
WINDOW = 128
LANES = 128
GROUP = 2
AHEAD = 2
TILE = 16
AXES = ("seq", "head")
LOG2E = 1.4426950408889634
MIB = 1 << 20
NT = (((1,), (1,)), ((), ()))
TN = (((0,), (0,)), ((), ()))
HBM = pl.BlockSpec(memory_space=pltpu.HBM)
VMEM = pl.BlockSpec(memory_space=pltpu.VMEM)
SMEM = pl.BlockSpec(memory_space=pltpu.SMEM)


def hbm(value):
    return pltpu.with_memory_space_constraint(value, pltpu.HBM)


def vmem(value):
    return pltpu.with_memory_space_constraint(value, pltpu.VMEM)


def pool_kernel(context_hbm, weight_hbm, pooled_ref, send_ref, context_ref, weight_ref, sem):
    blocks, width = pooled_ref.shape
    copies = (
        pltpu.make_async_copy(context_hbm, context_ref, sem.at[0]),
        pltpu.make_async_copy(weight_hbm, weight_ref, sem.at[1]),
    )
    for copy in copies:
        copy.start()
    for copy in copies:
        copy.wait()
    for block in range(blocks):
        entries = context_ref[pl.ds(block * POOL, POOL), :].astype(jnp.float32)
        pooled = jnp.sum(entries * weight_ref[...], axis=0, keepdims=True)
        pooled_ref[pl.ds(block, 1), :] = pooled
        normed = pooled * lax.rsqrt(jnp.mean(pooled * pooled, -1, keepdims=True) + 1e-06)
        lines = jnp.concatenate([normed[:, at : at + LANES] for at in range(0, width, LANES)], 0)
        if blocks == 1:
            send_ref[...] = jnp.broadcast_to(lines[None], send_ref.shape)
        else:
            for peer in range(send_ref.shape[0] // blocks):
                send_ref[peer * blocks + block] = lines


def finish_kernel(parts_ref, pooled_ref, weight_ref, out_ref):
    blocks, _ = pooled_ref.shape
    count, lines, lanes = parts_ref.shape
    total = jnp.sum(parts_ref[...].reshape(count // blocks, blocks, lines, lanes), 0)
    for block in range(blocks):
        grad = jnp.concatenate([total[block, j : j + 1] for j in range(lines)], 1)
        pooled = pooled_ref[pl.ds(block, 1), :]
        inverse = lax.rsqrt(jnp.mean(pooled * pooled, -1, keepdims=True) + 1e-06)
        normed = pooled * inverse
        grad = inverse * (grad - normed * jnp.mean(grad * normed, -1, keepdims=True))
        out_ref[pl.ds(block * POOL, POOL), :] = weight_ref[...] * grad


def load_kernel(cur_hbm, cur_ref, sem):
    copy = pltpu.make_async_copy(cur_hbm, cur_ref, sem)
    copy.start()
    copy.wait()


def fill_keys(comp_ref, prev_ref, window_ref, *keys_refs):
    count, lines, lanes = comp_ref.shape
    window_ref[pl.ds(0, WINDOW), :] = prev_ref[...]
    for line in range(lines):
        piece = comp_ref[:, line, :].astype(jnp.bfloat16)
        for keys_ref in keys_refs:
            keys_ref[pl.ds(0, count), pl.ds(line * lanes, lanes)] = piece


def score_kernel(
    heads, first_ref, q_hbm, c_hbm, comp_ref, prev_ref, cur_ref, p_ref, g_ref, sum_ref,
    q_ref, c_ref, window_ref, keys_ref, total_ref, sem,
):
    count, lines, lanes = comp_ref.shape
    rows, width = q_ref.shape
    part = TILE * heads
    group = min(GROUP, p_ref.shape[0])
    block = part * group
    steps = rows // block
    slab = TILE * group + WINDOW
    factor = width ** (-0.5)

    def fetch(step):
        span = pl.ds(pl.multiple_of(step * block, block), block)
        return (
            pltpu.make_async_copy(q_hbm.at[span], q_ref.at[span], sem.at[0, step]),
            pltpu.make_async_copy(c_hbm.at[span], c_ref.at[span], sem.at[1, step]),
        )

    for copy in fetch(0):
        copy.start()
    window_ref[pl.ds(WINDOW, cur_ref.shape[0]), :] = cur_ref[...]
    fill_keys(comp_ref, prev_ref, window_ref, keys_ref)
    total_ref[...] = jnp.zeros_like(total_ref)
    for step in range(1, min(AHEAD, steps)):
        for copy in fetch(step):
            copy.start()

    @pl.loop(0, steps, unroll=True)
    def _(step):
        start = pl.multiple_of(step * (TILE * group), TILE * group)
        keys_ref[pl.ds(count, slab), :] = window_ref[pl.ds(start, slab), :]
        for copy in fetch(step):
            copy.wait()

        @pl.when(step + AHEAD < steps)
        def _():
            for copy in fetch(step + AHEAD):
                copy.start()

        keys = keys_ref[...]
        span = pl.ds(pl.multiple_of(step * block, block), block)
        q = q_ref[span, :]
        c = c_ref[span, :]
        scores = lax.dot_general(keys, q, NT, preferred_element_type=jnp.float32)
        grads = lax.dot_general(keys, c, NT, preferred_element_type=jnp.float32)
        key = lax.broadcasted_iota(jnp.int32, (slab, block), 0)
        token = lax.broadcasted_iota(jnp.int32, (slab, block), 1) // heads
        low = jnp.where(first_ref[0] > 0, WINDOW - start, 0)
        valid = (key > token) & (key <= token + WINDOW) & (key >= low)
        scores = jnp.concatenate([scores[:count], jnp.where(valid, scores[count:], -1e30)], 0)
        peak = jnp.max(scores, 0, keepdims=True)
        weights = jnp.exp2((scores - peak) * (factor * LOG2E))
        probs = weights * (1.0 / jnp.sum(weights, 0, keepdims=True))
        half = probs.astype(jnp.bfloat16)
        delta = jnp.sum(half.astype(jnp.float32) * grads, 0, keepdims=True)
        slope = (probs * (grads - delta)).astype(jnp.bfloat16)
        for ref, value in ((p_ref, half), (g_ref, slope)):
            for index in range(group):
                columns = slice(index * part, (index + 1) * part)
                first = count + index * TILE
                ref[step * group + index, pl.ds(0, count), :] = value[:count, columns]
                window = value[first : first + TILE + WINDOW, columns]
                ref[step * group + index, pl.ds(count, TILE + WINDOW), :] = window
        total = jnp.dot(half[:count], c, preferred_element_type=jnp.float32)
        total += factor * jnp.dot(slope[:count], q, preferred_element_type=jnp.float32)
        total_ref[...] += total

    for line in range(lines):
        sum_ref[:, line, :] = total_ref[:, pl.ds(line * lanes, lanes)]


def output_kernel(
    p_ref, g_ref, comp_ref, prev_ref, cur_hbm, out_hbm, grad_hbm,
    out_ref, grad_ref, window_ref, keys_refs, sem, cur_sem,
):
    steps, _, block = p_ref.shape
    count = comp_ref.shape[0]
    factor = out_ref.shape[1] ** (-0.5)
    unroll = 2 if steps % 2 == 0 else 1

    def flush(step):
        rows = pl.ds(pl.multiple_of(step * block, block), block)
        return (
            pltpu.make_async_copy(out_ref.at[rows], out_hbm.at[rows], sem.at[0, step]),
            pltpu.make_async_copy(grad_ref.at[rows], grad_hbm.at[rows], sem.at[1, step]),
        )

    copy_cur = pltpu.make_async_copy(cur_hbm, window_ref.at[pl.ds(WINDOW, cur_hbm.shape[0])], cur_sem)
    copy_cur.start()
    fill_keys(comp_ref, prev_ref, window_ref, keys_refs.at[0], keys_refs.at[1])
    copy_cur.wait()

    @pl.loop(0, steps // unroll)
    def _(turn):
        for slot in range(unroll):
            step = turn * unroll + slot
            start = pl.multiple_of(step * TILE, TILE)
            keys_refs[slot, pl.ds(count, TILE + WINDOW), :] = window_ref[pl.ds(start, TILE + WINDOW), :]
            keys = keys_refs[slot]
            rows = pl.ds(pl.multiple_of(step * block, block), block)
            out = lax.dot_general(p_ref[step], keys, TN, preferred_element_type=jnp.float32)
            out_ref[rows, :] = out.astype(jnp.bfloat16)
            grad = lax.dot_general(g_ref[step], keys, TN, preferred_element_type=jnp.float32)
            grad_ref[rows, :] = (grad * factor).astype(jnp.bfloat16)
        for slot in range(unroll):
            for copy in flush(turn * unroll + slot):
                copy.start()

    for step in range(steps):
        for copy in flush(step):
            copy.wait()


def local(queries, cotangent, window_kv, context, pool_weight):
    tokens, heads, width = queries.shape
    blocks = context.shape[0] // POOL
    size = lax.axis_size("seq")
    count = size * lax.axis_size("head") * blocks
    rows = tokens * heads
    steps = tokens // TILE
    block = TILE * heads
    slab = count + TILE + WINDOW
    lines = width // LANES

    packed = jax.ShapeDtypeStruct((count, lines, LANES), jnp.float32)
    pooled, send = pl.pallas_call(
        pool_kernel,
        in_specs=[HBM, HBM],
        out_specs=(VMEM, VMEM),
        out_shape=(jax.ShapeDtypeStruct((blocks, width), jnp.float32), packed),
        scratch_shapes=[
            pltpu.VMEM(context.shape, context.dtype),
            pltpu.VMEM(pool_weight.shape, pool_weight.dtype),
            pltpu.SemaphoreType.DMA((2,)),
        ],
        name="pool",
        compiler_params=pltpu.CompilerParams(vmem_limit_bytes=8 * MIB),
    )(hbm(context), hbm(pool_weight))
    comp = lax.all_to_all(send, AXES, 0, 0, tiled=True)
    prev = lax.ppermute(window_kv[-WINDOW:], "seq", [(i, i + 1) for i in range(size - 1)])
    first = (lax.axis_index("seq") == 0).astype(jnp.int32).reshape(1)

    q = hbm(queries.reshape(rows, width))
    c = hbm(cotangent.reshape(rows, width))
    cur = hbm(window_kv)
    full = pltpu.VMEM((rows, width), jnp.bfloat16)
    kept = pltpu.VMEM((steps, slab, block), jnp.bfloat16)
    group = min(GROUP, steps)
    window = pltpu.VMEM((WINDOW + tokens, width), jnp.bfloat16)
    wide = pltpu.VMEM((count + TILE * group + WINDOW, width), jnp.bfloat16)
    total = pltpu.VMEM((count, width), jnp.float32)
    params = pltpu.CompilerParams(vmem_limit_bytes=32 * MIB)
    held = pl.pallas_call(
        load_kernel,
        in_specs=[HBM],
        out_specs=VMEM,
        out_shape=pltpu.VMEM(window_kv.shape, window_kv.dtype),
        scratch_shapes=[pltpu.SemaphoreType.DMA],
        cost_estimate=pl.CostEstimate(flops=10**9, bytes_accessed=2 * tokens * width, transcendentals=0),
        compiler_params=pltpu.CompilerParams(vmem_limit_bytes=4 * MIB),
        name="load",
    )(cur)
    half, slope, grad_comp = pl.pallas_call(
        functools.partial(score_kernel, heads),
        in_specs=[SMEM, HBM, HBM, VMEM, VMEM, VMEM],
        out_specs=(VMEM, VMEM, VMEM),
        out_shape=(kept, kept, packed),
        scratch_shapes=[full, full, window, wide, total, pltpu.SemaphoreType.DMA((2, steps // group))],
        cost_estimate=pl.CostEstimate(
            flops=4 * rows * slab * width + 4 * rows * count * width,
            bytes_accessed=4 * rows * (width + slab),
            transcendentals=rows * slab,
        ),
        compiler_params=params,
        name="score",
    )(first, q, c, comp, prev, vmem(held))
    parts = lax.all_to_all(grad_comp, AXES, 0, 0, tiled=True)
    out, grad = pl.pallas_call(
        output_kernel,
        in_specs=[VMEM, VMEM, VMEM, VMEM, HBM],
        out_specs=(HBM, HBM),
        out_shape=(jax.ShapeDtypeStruct((rows, width), jnp.bfloat16),) * 2,
        scratch_shapes=[full, full, window, pltpu.VMEM((2, slab, width), jnp.bfloat16), pltpu.SemaphoreType.DMA((2, steps)), pltpu.SemaphoreType.DMA],
        cost_estimate=pl.CostEstimate(
            flops=4 * rows * slab * width,
            bytes_accessed=4 * rows * (width + slab),
            transcendentals=0,
        ),
        compiler_params=params,
        name="outputs",
    )(vmem(half), vmem(slope), comp, prev, cur)
    grad_context = pl.pallas_call(
        finish_kernel,
        out_shape=jax.ShapeDtypeStruct(context.shape, jnp.float32),
        name="finish",
        compiler_params=pltpu.CompilerParams(vmem_limit_bytes=8 * MIB),
    )(parts, pooled, pool_weight)
    return out.reshape(queries.shape), grad.reshape(queries.shape), grad_context


def solution(mesh):
    in_specs = (
        P("seq", "head", None),
        P("seq", "head", None),
        P("seq", None),
        P(("seq", "head"), None),
        P(),
    )
    out_specs = (P("seq", "head", None), P("seq", "head", None), P(("seq", "head"), None))

    return jax.shard_map(local, mesh=mesh, in_specs=in_specs, out_specs=out_specs, check_vma=False)
```
